32 devices in a mesh: rows: 8 (over z, y), rep: 4 (over x, core).
Axes of the slice: x: 2, y: 2, z: 4, core: 2. Of those that a mesh axis runs over, the one named last changes fastest.
Arguments:
- binned: int32 [8192, 1024], P('rows', 'rep'), may hold values from 0 to 127
- gradients: bfloat16 [8192], P('rows'), may hold values from -3 to 3
- hessians: bfloat16 [8192], P('rows'), may hold values from 0.019897461 to 0.25
- parents: int32 [8192], P('rows'), may hold values from 0 to 15
- split_feature: int32 [16], replicated, may hold values from 0 to 1023
- split_bin: int32 [16], replicated, may hold values from 32 to 95
- elected: int32 [32, 512], P(None, 'rep'), may hold values from 0 to 255
Outputs:
- new_nodes: int32 [8192], P('rows')
- best_gain: float32 [32, 4, 128], P(None, 'rep', 'rows')
- node_best: float32 [32], replicated
The draws below stay inside these ranges and needn't reach their ends.
All inputs are finite; a program needn't handle non-finite values.
Results may differ from the reference program's by a relative error of at most 0.0003.
Values sent between devices are 32-bit elements; how exact they have to be, the bound alone decides.
A program may use at most 64 MiB of HBM per device.

```python
import math
import jax
import jax.numpy as jnp

F = 1024
BINS = 128
ELECT = 512
NODES = 32
PARENTS = 16
ROWS = 8192
N_REP = 4


def plant(result, key, least, largest):
    longest = result.shape.index(max(result.shape))
    spots = []
    for shift in (0, 1):
        where = [jax.random.randint(jax.random.fold_in(key, axis), (), 0, length) for axis, length in enumerate(result.shape)]
        where[longest] = (where[longest] + shift) % result.shape[longest]
        spots.append(tuple(where))
    return result.at[spots[0]].set(least).at[spots[1]].set(largest)


def level_of(rng, shape, cuts, least, high):
    def one(axis_at, blocks):
        steps = jax.random.uniform(jax.random.fold_in(jax.random.fold_in(rng, 6), axis_at), (blocks,), jnp.float32, least / len(cuts), high / len(cuts))
        return jnp.repeat(jnp.exp(steps), shape[axis_at] // blocks).reshape((-1,) + (1,) * (len(shape) - axis_at - 1))

    level = one(*cuts[0])
    for cut in cuts[1:]:
        level = level * one(*cut)
    return level


def centred(own_key, extent, deviation, bound, pieces=(), kind=jnp.bfloat16):
    loudness = level_of(own_key, extent, pieces, -0.22, 0.18) if pieces else 1.0
    drawn = jax.random.normal(own_key, extent, jnp.float32) * deviation * loudness
    return jnp.minimum(jnp.maximum(drawn, -bound), bound).astype(kind)


def setup_inputs(seed: int = 0) -> dict:
    seeds = jax.random.split(jax.random.key(seed), 8)
    return {
        "binned": plant(jax.random.randint(seeds[0], (ROWS, F), 0, BINS), jax.random.fold_in(seeds[0], 1), 0, BINS - 1).astype(jnp.int32),
        "gradients": centred(seeds[1], (ROWS,), 0.5, 3.0, ((0, 8),)),
        "hessians": jnp.clip(jnp.exp(math.log(0.25) - 2.5308688 * jax.random.uniform(seeds[2], (ROWS,), jnp.float32) ** level_of(seeds[2], (ROWS,), ((0, 8),), -0.2, 0.2)), 0.019897461, 0.25).astype(jnp.bfloat16),
        "parents": plant(jax.random.randint(seeds[3], (ROWS,), 0, PARENTS), jax.random.fold_in(seeds[3], 1), 0, PARENTS - 1).astype(jnp.int32),
        "split_feature": plant(jax.random.randint(seeds[4], (PARENTS,), 0, F), jax.random.fold_in(seeds[4], 1), 0, F - 1).astype(jnp.int32),
        "split_bin": plant(jax.random.randint(seeds[5], (PARENTS,), BINS // 4, 3 * BINS // 4), jax.random.fold_in(seeds[5], 1), BINS // 4, (3 * BINS // 4) - 1).astype(jnp.int32),
        "elected": plant(jax.random.randint(seeds[6], (NODES, ELECT), 0, F // N_REP), jax.random.fold_in(seeds[6], 1), 0, (F // N_REP) - 1).astype(jnp.int32),
    }


l2_penalty = 1.0


def reference(binned, gradients, hessians, parents, split_feature, split_bin, elected):
    row_feature = split_feature[parents]
    row_value = jnp.take_along_axis(binned, row_feature[:, None], axis=1)[:, 0]
    side_bits = (row_value > split_bin[parents]).astype(jnp.int32)
    new_nodes = (2 * parents + side_bits).astype(jnp.int32)
    slot_ids = jnp.arange(ELECT, dtype=jnp.int32)
    block_start = (slot_ids // (ELECT // N_REP)) * (F // N_REP)
    feature = (elected + block_start[None, :]).astype(jnp.int32)
    row_features = feature[new_nodes]
    row_bins = jnp.take_along_axis(binned, row_features, axis=1)
    segment = (new_nodes[:, None] * ELECT + slot_ids[None, :]) * BINS + row_bins
    segment = segment.astype(jnp.int32).reshape(-1)
    grad_wide = gradients.astype(jnp.float32)
    hess_wide = hessians.astype(jnp.float32)
    count = NODES * ELECT * BINS
    hist_grad = jax.ops.segment_sum(jnp.broadcast_to(grad_wide[:, None], row_bins.shape).reshape(-1), segment, num_segments=count).reshape(NODES, ELECT, BINS)
    hist_hess = jax.ops.segment_sum(jnp.broadcast_to(hess_wide[:, None], row_bins.shape).reshape(-1), segment, num_segments=count).reshape(NODES, ELECT, BINS)
    total_grad = jax.ops.segment_sum(grad_wide, new_nodes, num_segments=NODES)[:, None, None]
    total_hess = jax.ops.segment_sum(hess_wide, new_nodes, num_segments=NODES)[:, None, None]
    left_grad = jnp.cumsum(hist_grad, axis=2)[:, :, :-1]
    left_hess = jnp.cumsum(hist_hess, axis=2)[:, :, :-1]
    split_gain = 0.5 * (left_grad * left_grad / (left_hess + l2_penalty)
                        + (total_grad - left_grad) ** 2 / (total_hess - left_hess + l2_penalty)
                        - total_grad * total_grad / (total_hess + l2_penalty))
    best_slot = jnp.max(split_gain, axis=2)
    best_gain = best_slot.reshape(NODES, N_REP, ELECT // N_REP)
    node_best = jnp.max(best_slot, axis=1)
    return new_nodes, best_gain, node_best
```

```python
import functools

import jax
import jax.numpy as jnp
from jax import lax
from jax.experimental import pallas as pl
from jax.experimental.pallas import tpu as pltpu
from jax.sharding import PartitionSpec as P

BINS = 128
LANES = 128
MESH = pl.DeviceIdType.MESH

l2_penalty = 1.0


def kernel(
    n_rows, n_rep,
    split_feature, split_bin, binned, gh, parents, elected,
    new_nodes, best_out, node_best,
    side_snd, side_rcv, bins_snd, bins_rcv, node_rcv, gh_rcv, le, acc, top_snd, top_rcv, all_snd, all_rcv,
    side_ss, side_rs, gh_ss, gh_rs, node_ss, node_rs, bins_ss, bins_rs, top_ss, top_rs, all_ss, all_rs,
):
    rows_here, block_width = binned.shape
    node_count, slots_here = elected.shape
    parent_count = split_feature.shape[0]
    owned = slots_here // n_rows
    me = lax.axis_index("rows")
    rep = lax.axis_index("rep")

    def at_row(d):
        return (lax.rem(me + d, n_rows), rep)

    def at_rep(d):
        return (me, lax.rem(rep + d, n_rep))

    def send(src, dst, ss, rs, device):
        copy = pltpu.make_async_remote_copy(
            src_ref=src, dst_ref=dst, send_sem=ss, recv_sem=rs, device_id=device, device_id_type=MESH
        )
        copy.start()
        return copy

    barrier = pltpu.get_barrier_semaphore()
    for d in range(1, n_rep):
        pl.semaphore_signal(barrier, inc=1, device_id=at_rep(d), device_id_type=MESH)
    for d in range(1, n_rows):
        pl.semaphore_signal(barrier, inc=1, device_id=at_row(d), device_id_type=MESH)

    parent_sub = lax.broadcasted_iota(jnp.int32, (parent_count, block_width), 0)
    column = lax.broadcasted_iota(jnp.int32, (parent_count, block_width), 1) + rep * block_width
    feature_of = jnp.zeros((parent_count, block_width), jnp.int32)
    parent_row = lax.broadcasted_iota(jnp.int32, (parent_count, rows_here), 0)
    bin_of = jnp.zeros((parent_count, rows_here), jnp.int32)
    owns = jnp.zeros((parent_count, rows_here), jnp.int32)
    low = rep * block_width
    for p in range(parent_count):
        feature = split_feature[p]
        owned_here = jnp.where((feature >= low) & (feature < low + block_width), 1, 0)
        feature_of = jnp.where(parent_sub == p, feature, feature_of)
        bin_of = jnp.where(parent_row == p, split_bin[p], bin_of)
        owns = jnp.where(parent_row == p, owned_here, owns)
    picks = jnp.where(feature_of == column, 1.0, 0.0).astype(jnp.bfloat16)
    values = lax.dot_general(
        picks,
        binned[...].astype(jnp.float32).astype(jnp.bfloat16),
        (((1,), (1,)), ((), ())),
        preferred_element_type=jnp.float32,
    )
    own_parents = parents[...]
    goes = (parent_row == own_parents) & (owns > 0) & (values > bin_of.astype(jnp.float32))
    side = jnp.sum(jnp.where(goes, 1.0, 0.0), axis=0, keepdims=True)
    side_snd[...] = side

    pl.semaphore_wait(barrier, n_rep + n_rows - 2)
    copies = []
    for d in range(1, n_rep):
        copies.append(send(side_snd, side_rcv.at[d], side_ss.at[d], side_rs.at[d], at_rep(d)))
    for d in range(1, n_rows):
        copies.append(send(gh, gh_rcv.at[d], gh_ss.at[d], gh_rs.at[d], at_row(d)))
    gh_rcv[0] = gh[...]
    for d in range(1, n_rep):
        copies[d - 1].wait_recv()
        side = side + side_rcv[d]
    nodes = 2 * own_parents + side.astype(jnp.int32)
    new_nodes[...] = nodes
    node_rcv[0] = nodes

    node_sub = lax.broadcasted_iota(jnp.int32, (node_count, rows_here), 0)
    node_hot = jnp.where(node_sub == nodes, 1.0, 0.0).astype(jnp.bfloat16)
    index = lax.dot_general(
        node_hot,
        elected[...].astype(jnp.float32).astype(jnp.bfloat16),
        (((0,), (0,)), ((), ())),
        preferred_element_type=jnp.float32,
    ).astype(jnp.int32)
    lane = index % LANES
    part = index // LANES
    chosen = None
    for start in range(block_width // LANES):
        piece = binned[:, start * LANES : (start + 1) * LANES]
        found = jnp.take_along_axis(piece, lane, axis=1, mode="promise_in_bounds")
        chosen = found if chosen is None else jnp.where(part == start, found, chosen)
    turned = chosen.astype(jnp.float32).T
    for j in range(n_rows):
        bins_snd[j] = turned[j * owned : (j + 1) * owned]
    for d in range(1, n_rows):
        send(node_rcv.at[0], node_rcv.at[d], node_ss.at[d], node_rs.at[d], at_row(d))
        send(bins_snd.at[lax.rem(me + d, n_rows)], bins_rcv.at[d], bins_ss.at[d], bins_rs.at[d], at_row(d))
    bins_rcv[0] = bins_snd[me]

    def wait_for(d):
        for src, dst, ss, rs in (
            (gh, gh_rcv, gh_ss, gh_rs),
            (node_rcv.at[0], node_rcv, node_ss, node_rs),
            (bins_snd.at[0], bins_rcv, bins_ss, bins_rs),
        ):
            pltpu.make_async_remote_copy(
                src_ref=src, dst_ref=dst.at[d], send_sem=ss.at[d], recv_sem=rs.at[d],
                device_id=at_row(d), device_id_type=MESH,
            ).wait()

    bin_sub = lax.broadcasted_iota(jnp.int32, (BINS, rows_here), 0).astype(jnp.float32).astype(jnp.bfloat16)

    def add_source(d):
        there = node_sub == node_rcv[d]
        weights = jnp.concatenate(
            [jnp.where(there, gh_rcv[d, 0:1], 0.0), jnp.where(there, gh_rcv[d, 1:2], 0.0)], axis=0
        ).astype(jnp.bfloat16)
        bins = bins_rcv[d].astype(jnp.bfloat16)
        one = jnp.ones((), jnp.bfloat16)
        none = jnp.zeros((), jnp.bfloat16)
        for k in range(owned):
            le[k * BINS : (k + 1) * BINS, :] = jnp.where(bins[k : k + 1] <= bin_sub, one, none)
        return lax.dot_general(le[...], weights, (((1,), (1,)), ((), ())), preferred_element_type=jnp.float32)

    acc[...] = add_source(0)

    @pl.loop(1, n_rows)
    def _(d):
        wait_for(d)
        acc[...] += add_source(d)

    below = lax.broadcasted_iota(jnp.int32, (BINS, node_count), 0) < BINS - 1
    best = None
    for k in range(owned):
        left_grad = acc[k * BINS : (k + 1) * BINS, 0:node_count]
        left_hess = acc[k * BINS : (k + 1) * BINS, node_count : 2 * node_count]
        total_grad = left_grad[BINS - 1 : BINS]
        total_hess = left_hess[BINS - 1 : BINS]
        right_grad = total_grad - left_grad
        gain = 0.5 * (
            left_grad * left_grad / (left_hess + l2_penalty)
            + right_grad * right_grad / (total_hess - left_hess + l2_penalty)
            - total_grad * total_grad / (total_hess + l2_penalty)
        )
        top = jnp.max(jnp.where(below, gain, -jnp.inf), axis=0, keepdims=True)
        best_out[k : k + 1, :] = top
        best = top if best is None else jnp.maximum(best, top)

    def share(snd, rcv, ss, rs, size, at, value):
        snd[...] = value
        sent = [send(snd, rcv.at[d], ss.at[d], rs.at[d], at(d)) for d in range(1, size)]
        for d in range(1, size):
            sent[d - 1].wait()
            value = jnp.maximum(value, rcv[d])
        return value

    best = share(top_snd, top_rcv, top_ss, top_rs, n_rows, at_row, best)
    best = share(all_snd, all_rcv, all_ss, all_rs, n_rep, at_rep, best)
    node_best[...] = best
    for d in range(1, n_rep):
        copies[d - 1].wait_send()


def body(n_rows, n_rep, binned, gradients, hessians, parents, split_feature, split_bin, elected):
    rows_here, block_width = binned.shape
    node_count, slots_here = elected.shape
    owned = slots_here // n_rows
    f32 = jnp.float32
    gh = jnp.stack([gradients, hessians]).astype(f32)
    vmem = pl.BlockSpec(memory_space=pltpu.VMEM)
    smem = pl.BlockSpec(memory_space=pltpu.SMEM)
    dma = pltpu.SemaphoreType.DMA
    new_nodes, best, node_best = pl.pallas_call(
        functools.partial(kernel, n_rows, n_rep),
        out_shape=(
            jax.ShapeDtypeStruct((1, rows_here), jnp.int32),
            jax.ShapeDtypeStruct((owned, node_count), f32),
            jax.ShapeDtypeStruct((1, node_count), f32),
        ),
        in_specs=[smem, smem, vmem, vmem, vmem, vmem],
        out_specs=(vmem, vmem, vmem),
        scratch_shapes=[
            pltpu.VMEM((1, rows_here), f32),
            pltpu.VMEM((n_rep, 1, rows_here), f32),
            pltpu.VMEM((n_rows, owned, rows_here), f32),
            pltpu.VMEM((n_rows, owned, rows_here), f32),
            pltpu.VMEM((n_rows, 1, rows_here), jnp.int32),
            pltpu.VMEM((n_rows, 2, rows_here), f32),
            pltpu.VMEM((owned * BINS, rows_here), jnp.bfloat16),
            pltpu.VMEM((owned * BINS, 2 * node_count), f32),
            pltpu.VMEM((1, node_count), f32),
            pltpu.VMEM((n_rows, 1, node_count), f32),
            pltpu.VMEM((1, node_count), f32),
            pltpu.VMEM((n_rep, 1, node_count), f32),
        ]
        + [dma((n_rep,))] * 2 + [dma((n_rows,))] * 8 + [dma((n_rep,))] * 2,
        compiler_params=pltpu.CompilerParams(collective_id=0, has_side_effects=True),
    )(split_feature, split_bin, binned, gh, parents.reshape(1, rows_here), elected)
    return (
        new_nodes.reshape(rows_here),
        best.T.reshape(node_count, 1, owned),
        node_best.reshape(node_count),
    )


def solution(mesh):
    return jax.shard_map(
        functools.partial(body, mesh.shape["rows"], mesh.shape["rep"]),
        mesh=mesh,
        in_specs=(P("rows", "rep"), P("rows"), P("rows"), P("rows"), P(), P(), P(None, "rep")),
        out_specs=(P("rows"), P(None, "rep", "rows"), P()),
        check_vma=False,
    )
```

```python
import functools

import jax
import jax.numpy as jnp
from jax import lax
from jax.experimental import pallas as pl
from jax.experimental.pallas import tpu as pltpu
from jax.sharding import PartitionSpec as P

BINS = 128
LANES = 128
MESH = pl.DeviceIdType.MESH

l2_penalty = 1.0


def kernel(
    n_rows, n_rep,
    split_feature_in, split_bin_in, binned_in, gradients_in, hessians_in, parents_in, elected_in,
    new_nodes, best_out, node_best,
    split_feature, split_bin, binned, gradients, hessians, parents, elected, in_sems, gh, left_bins, right_bins,
    side_snd, side_rcv, bins_snd, bins_rcv, node_rcv, gh_rcv, le, acc, top_snd, top_rcv, all_snd, all_rcv,
    side_ss, side_rs, gh_ss, gh_rs, node_ss, node_rs, bins_ss, bins_rs, top_ss, top_rs, all_ss, all_rs,
):
    rows_here, block_width = binned.shape
    node_count, slots_here = elected.shape
    parent_count = split_feature.shape[0]
    owned = slots_here // n_rows
    me = lax.axis_index("rows")
    rep = lax.axis_index("rep")

    def partner(d):
        if n_rows & (n_rows - 1):
            return lax.rem(me + d, n_rows) if d else me
        other = me
        for bit in range(n_rows.bit_length()):
            if d >> bit & 1:
                other = other + (1 - 2 * lax.rem(me // 2**bit, 2)) * 2**bit
        return other

    def at_row(d):
        return (partner(d), rep)

    def at_rep(d):
        return (me, lax.rem(rep + d, n_rep))

    def send(src, dst, ss, rs, device):
        copy = pltpu.make_async_remote_copy(
            src_ref=src, dst_ref=dst, send_sem=ss, recv_sem=rs, device_id=device, device_id_type=MESH
        )
        copy.start()
        return copy

    barrier = pltpu.get_barrier_semaphore()
    for d in range(1, n_rep):
        pl.semaphore_signal(barrier, inc=1, device_id=at_rep(d), device_id_type=MESH)
    for d in range(1, n_rows):
        pl.semaphore_signal(barrier, inc=1, device_id=at_row(d), device_id_type=MESH)

    loads = []
    for i, (src, dst) in enumerate(
        (
            (binned_in, binned), (split_feature_in, split_feature), (split_bin_in, split_bin), (parents_in, parents),
            (elected_in, elected), (gradients_in, gradients), (hessians_in, hessians),
        )
    ):
        loads.append(pltpu.make_async_copy(src, dst, in_sems.at[i]))
        loads[-1].start()
    for load in loads:
        load.wait()
    gh[0:1] = gradients[...].astype(jnp.float32).reshape(1, rows_here)
    gh[1:2] = hessians[...].astype(jnp.float32).reshape(1, rows_here)

    parent_sub = lax.broadcasted_iota(jnp.int32, (parent_count, block_width), 0)
    column = lax.broadcasted_iota(jnp.int32, (parent_count, block_width), 1) + rep * block_width
    feature_of = jnp.zeros((parent_count, block_width), jnp.int32)
    parent_row = lax.broadcasted_iota(jnp.int32, (parent_count, rows_here), 0)
    bin_of = jnp.zeros((parent_count, rows_here), jnp.int32)
    owns = jnp.zeros((parent_count, rows_here), jnp.int32)
    low = rep * block_width
    for p in range(parent_count):
        feature = split_feature[p]
        owned_here = jnp.where((feature >= low) & (feature < low + block_width), 1, 0)
        feature_of = jnp.where(parent_sub == p, feature, feature_of)
        bin_of = jnp.where(parent_row == p, split_bin[p], bin_of)
        owns = jnp.where(parent_row == p, owned_here, owns)
    picks = jnp.where(feature_of == column, 1.0, 0.0).astype(jnp.bfloat16)
    values = lax.dot_general(
        picks,
        binned[...].astype(jnp.float32).astype(jnp.bfloat16),
        (((1,), (1,)), ((), ())),
        preferred_element_type=jnp.float32,
    )
    own_parents = parents[...]
    goes = (parent_row == own_parents) & (owns > 0) & (values > bin_of.astype(jnp.float32))
    side = jnp.sum(jnp.where(goes, 1.0, 0.0), axis=0, keepdims=True)
    side_snd[...] = side

    node_sub = lax.broadcasted_iota(jnp.int32, (node_count, rows_here), 0)
    elected_wide = elected[...].astype(jnp.float32).astype(jnp.bfloat16)
    for child, turned in ((0, left_bins), (1, right_bins)):
        child_hot = jnp.where(node_sub == 2 * own_parents + child, 1.0, 0.0).astype(jnp.bfloat16)
        index = lax.dot_general(
            child_hot, elected_wide, (((0,), (0,)), ((), ())), preferred_element_type=jnp.float32
        ).astype(jnp.int32)
        lane = index % LANES
        part = index // LANES
        chosen = None
        for start in range(block_width // LANES):
            piece = binned[:, start * LANES : (start + 1) * LANES]
            found = jnp.take_along_axis(piece, lane, axis=1, mode="promise_in_bounds")
            chosen = found if chosen is None else jnp.where(part == start, found, chosen)
        turned[...] = chosen.astype(jnp.float32).T

    pl.semaphore_wait(barrier, n_rep + n_rows - 2)
    copies = []
    for d in range(1, n_rep):
        copies.append(send(side_snd, side_rcv.at[d], side_ss.at[d], side_rs.at[d], at_rep(d)))
    for d in range(1, n_rows):
        copies.append(send(gh, gh_rcv.at[d], gh_ss.at[d], gh_rs.at[d], at_row(d)))
    gh_rcv[0] = gh[...]
    for d in range(1, n_rep):
        copies[d - 1].wait_recv()
        side = side + side_rcv[d]
    nodes = 2 * own_parents + side.astype(jnp.int32)
    new_nodes[...] = nodes
    node_rcv[0] = nodes

    for j in range(n_rows):
        slots = slice(j * owned, (j + 1) * owned)
        bins_snd[j] = jnp.where(side > 0.5, right_bins[slots, :], left_bins[slots, :])
    for d in range(1, n_rows):
        send(node_rcv.at[0], node_rcv.at[d], node_ss.at[d], node_rs.at[d], at_row(d))
        send(bins_snd.at[partner(d)], bins_rcv.at[d], bins_ss.at[d], bins_rs.at[d], at_row(d))
    bins_rcv[0] = bins_snd[me]

    def wait_for(d):
        for src, dst, ss, rs in (
            (gh, gh_rcv, gh_ss, gh_rs),
            (node_rcv.at[0], node_rcv, node_ss, node_rs),
            (bins_snd.at[0], bins_rcv, bins_ss, bins_rs),
        ):
            pltpu.make_async_remote_copy(
                src_ref=src, dst_ref=dst.at[d], send_sem=ss.at[d], recv_sem=rs.at[d],
                device_id=at_row(1), device_id_type=MESH,
            ).wait()

    bin_sub = lax.broadcasted_iota(jnp.int32, (BINS, rows_here), 0).astype(jnp.float32).astype(jnp.bfloat16)

    def add_source(d):
        there = node_sub == node_rcv[d]
        weights = jnp.concatenate(
            [jnp.where(there, gh_rcv[d, 0:1], 0.0), jnp.where(there, gh_rcv[d, 1:2], 0.0)], axis=0
        ).astype(jnp.bfloat16)
        bins = bins_rcv[d].astype(jnp.bfloat16)
        one = jnp.ones((), jnp.bfloat16)
        none = jnp.zeros((), jnp.bfloat16)
        for k in range(owned):
            le[k * BINS : (k + 1) * BINS, :] = jnp.where(bins[k : k + 1] <= bin_sub, one, none)
        return lax.dot_general(le[...], weights, (((1,), (1,)), ((), ())), preferred_element_type=jnp.float32)

    acc[...] = add_source(0)

    @pl.loop(1, n_rows)
    def _(d):
        wait_for(d)
        acc[...] += add_source(d)

    below = lax.broadcasted_iota(jnp.int32, (BINS, node_count), 0) < BINS - 1
    best = None
    for k in range(owned):
        left_grad = acc[k * BINS : (k + 1) * BINS, 0:node_count]
        left_hess = acc[k * BINS : (k + 1) * BINS, node_count : 2 * node_count]
        total_grad = left_grad[BINS - 1 : BINS]
        total_hess = left_hess[BINS - 1 : BINS]
        right_grad = total_grad - left_grad
        gain = 0.5 * (
            left_grad * left_grad / (left_hess + l2_penalty)
            + right_grad * right_grad / (total_hess - left_hess + l2_penalty)
            - total_grad * total_grad / (total_hess + l2_penalty)
        )
        top = jnp.max(jnp.where(below, gain, -jnp.inf), axis=0, keepdims=True)
        best_out[k : k + 1, :] = top
        best = top if best is None else jnp.maximum(best, top)

    def share(snd, rcv, ss, rs, size, at, value):
        snd[...] = value
        sent = [send(snd, rcv.at[d], ss.at[d], rs.at[d], at(d)) for d in range(1, size)]
        for d in range(1, size):
            sent[d - 1].wait()
            value = jnp.maximum(value, rcv[d])
        return value

    best = share(top_snd, top_rcv, top_ss, top_rs, n_rows, at_row, best)
    best = share(all_snd, all_rcv, all_ss, all_rs, n_rep, at_rep, best)
    node_best[...] = best
    for d in range(1, n_rep):
        copies[d - 1].wait_send()


def hand_on(*refs):
    for src, dst in zip(refs[:3], refs[3:]):
        dst[...] = src[...]


def body(n_rows, n_rep, binned, gradients, hessians, parents, split_feature, split_bin, elected):
    rows_here, block_width = binned.shape
    node_count, slots_here = elected.shape
    owned = slots_here // n_rows
    f32 = jnp.float32
    vmem = pl.BlockSpec(memory_space=pltpu.VMEM)
    dma = pltpu.SemaphoreType.DMA
    new_nodes, best, node_best = pl.pallas_call(
        functools.partial(kernel, n_rows, n_rep),
        out_shape=(
            jax.ShapeDtypeStruct((1, rows_here), jnp.int32),
            jax.ShapeDtypeStruct((owned, node_count), f32),
            jax.ShapeDtypeStruct((1, node_count), f32),
        ),
        in_specs=[pl.BlockSpec(memory_space=pl.ANY)] * 7,
        out_specs=(vmem, vmem, vmem),
        scratch_shapes=[
            pltpu.SMEM(split_feature.shape, jnp.int32),
            pltpu.SMEM(split_bin.shape, jnp.int32),
            pltpu.VMEM(binned.shape, jnp.int32),
            pltpu.VMEM(gradients.shape, gradients.dtype),
            pltpu.VMEM(hessians.shape, hessians.dtype),
            pltpu.VMEM((1, rows_here), jnp.int32),
            pltpu.VMEM(elected.shape, jnp.int32),
            dma((7,)),
            pltpu.VMEM((2, rows_here), f32),
            pltpu.VMEM((slots_here, rows_here), f32),
            pltpu.VMEM((slots_here, rows_here), f32),
            pltpu.VMEM((1, rows_here), f32),
            pltpu.VMEM((n_rep, 1, rows_here), f32),
            pltpu.VMEM((n_rows, owned, rows_here), f32),
            pltpu.VMEM((n_rows, owned, rows_here), f32),
            pltpu.VMEM((n_rows, 1, rows_here), jnp.int32),
            pltpu.VMEM((n_rows, 2, rows_here), f32),
            pltpu.VMEM((owned * BINS, rows_here), jnp.bfloat16),
            pltpu.VMEM((owned * BINS, 2 * node_count), f32),
            pltpu.VMEM((1, node_count), f32),
            pltpu.VMEM((n_rows, 1, node_count), f32),
            pltpu.VMEM((1, node_count), f32),
            pltpu.VMEM((n_rep, 1, node_count), f32),
        ]
        + [dma((n_rep,))] * 2 + [dma((n_rows,))] * 8 + [dma((n_rep,))] * 2,
        compiler_params=pltpu.CompilerParams(collective_id=0, has_side_effects=True),
    )(split_feature, split_bin, binned, gradients, hessians, parents.reshape(1, rows_here), elected)
    made = (new_nodes, best, node_best)
    new_nodes, best, node_best = pl.pallas_call(
        hand_on,
        out_shape=tuple(jax.ShapeDtypeStruct(a.shape, a.dtype) for a in made),
        in_specs=[vmem] * 3,
        out_specs=(vmem,) * 3,
    )(*made)
    return (
        new_nodes.reshape(rows_here),
        best.T.reshape(node_count, 1, owned),
        node_best.reshape(node_count),
    )


def solution(mesh):
    return jax.shard_map(
        functools.partial(body, mesh.shape["rows"], mesh.shape["rep"]),
        mesh=mesh,
        in_specs=(P("rows", "rep"), P("rows"), P("rows"), P("rows"), P(), P(), P(None, "rep")),
        out_specs=(P("rows"), P(None, "rep", "rows"), P()),
        check_vma=False,
    )
```

```python
import functools

import jax
import jax.numpy as jnp
from jax import lax
from jax.experimental import pallas as pl
from jax.experimental.pallas import tpu as pltpu
from jax.sharding import PartitionSpec as P

BINS = 128
LANES = 128
MESH = pl.DeviceIdType.MESH

l2_penalty = 1.0


def kernel(
    n_rows, n_rep,
    split_feature_in, split_bin_in, binned_in, gradients_in, hessians_in, parents_in, elected_in,
    new_nodes, best_out, node_best,
    split_feature, split_bin, binned, gradients, hessians, parents, elected, in_sems, gh, left_bins, right_bins,
    side_snd, side_rcv, bins_snd, bins_rcv, node_rcv, gh_rcv, le, acc, top_snd, top_rcv,
    side_ss, side_rs, gh_ss, gh_rs, node_ss, node_rs, bins_ss, bins_rs, top_ss, top_rs,
):
    rows_here, block_width = binned.shape
    node_count, slots_here = elected.shape
    parent_count = split_feature.shape[0]
    owned = slots_here // n_rows
    me = lax.axis_index("rows")
    rep = lax.axis_index("rep")

    def partner(d):
        if n_rows & (n_rows - 1):
            return lax.rem(me + d, n_rows) if d else me
        other = me
        for bit in range(n_rows.bit_length()):
            if d >> bit & 1:
                other = other + (1 - 2 * lax.rem(me // 2**bit, 2)) * 2**bit
        return other

    def at_row(d):
        return (partner(d), rep)

    def at_rep(d):
        return (me, lax.rem(rep + d, n_rep))

    def send(src, dst, ss, rs, device):
        copy = pltpu.make_async_remote_copy(
            src_ref=src, dst_ref=dst, send_sem=ss, recv_sem=rs, device_id=device, device_id_type=MESH
        )
        copy.start()
        return copy

    barrier = pltpu.get_barrier_semaphore()
    others = [(d, e) for d in range(n_rows) for e in range(n_rep) if d or e]

    def at(d, e):
        return (partner(d), lax.rem(rep + e, n_rep))

    for d, e in others:
        pl.semaphore_signal(barrier, inc=1, device_id=at(d, e), device_id_type=MESH)

    loads = []
    for i, (src, dst) in enumerate(
        (
            (binned_in, binned), (split_feature_in, split_feature), (split_bin_in, split_bin), (parents_in, parents),
            (elected_in, elected), (gradients_in, gradients), (hessians_in, hessians),
        )
    ):
        loads.append(pltpu.make_async_copy(src, dst, in_sems.at[i]))
        loads[-1].start()
    for load in loads:
        load.wait()
    gh[0:1] = gradients[...].astype(jnp.float32).reshape(1, rows_here)
    gh[1:2] = hessians[...].astype(jnp.float32).reshape(1, rows_here)

    parent_sub = lax.broadcasted_iota(jnp.int32, (parent_count, block_width), 0)
    column = lax.broadcasted_iota(jnp.int32, (parent_count, block_width), 1) + rep * block_width
    feature_of = jnp.zeros((parent_count, block_width), jnp.int32)
    parent_row = lax.broadcasted_iota(jnp.int32, (parent_count, rows_here), 0)
    bin_of = jnp.zeros((parent_count, rows_here), jnp.int32)
    owns = jnp.zeros((parent_count, rows_here), jnp.int32)
    low = rep * block_width
    for p in range(parent_count):
        feature = split_feature[p]
        owned_here = jnp.where((feature >= low) & (feature < low + block_width), 1, 0)
        feature_of = jnp.where(parent_sub == p, feature, feature_of)
        bin_of = jnp.where(parent_row == p, split_bin[p], bin_of)
        owns = jnp.where(parent_row == p, owned_here, owns)
    picks = jnp.where(feature_of == column, 1.0, 0.0).astype(jnp.bfloat16)
    values = lax.dot_general(
        picks,
        binned[...].astype(jnp.float32).astype(jnp.bfloat16),
        (((1,), (1,)), ((), ())),
        preferred_element_type=jnp.float32,
    )
    own_parents = parents[...]
    goes = (parent_row == own_parents) & (owns > 0) & (values > bin_of.astype(jnp.float32))
    side = jnp.sum(jnp.where(goes, 1.0, 0.0), axis=0, keepdims=True)
    side_snd[...] = side

    node_sub = lax.broadcasted_iota(jnp.int32, (node_count, rows_here), 0)
    elected_wide = elected[...].astype(jnp.float32).astype(jnp.bfloat16)
    for child, turned in ((0, left_bins), (1, right_bins)):
        child_hot = jnp.where(node_sub == 2 * own_parents + child, 1.0, 0.0).astype(jnp.bfloat16)
        index = lax.dot_general(
            child_hot, elected_wide, (((0,), (0,)), ((), ())), preferred_element_type=jnp.float32
        ).astype(jnp.int32)
        lane = index % LANES
        part = index // LANES
        chosen = None
        for start in range(block_width // LANES):
            piece = binned[:, start * LANES : (start + 1) * LANES]
            found = jnp.take_along_axis(piece, lane, axis=1, mode="promise_in_bounds")
            chosen = found if chosen is None else jnp.where(part == start, found, chosen)
        turned[...] = chosen.astype(jnp.float32).T

    pl.semaphore_wait(barrier, len(others))
    copies = []
    for d in range(1, n_rep):
        copies.append(send(side_snd, side_rcv.at[d], side_ss.at[d], side_rs.at[d], at_rep(d)))
    for d in range(1, n_rows):
        copies.append(send(gh, gh_rcv.at[d], gh_ss.at[d], gh_rs.at[d], at_row(d)))
    gh_rcv[0] = gh[...]
    for d in range(1, n_rep):
        copies[d - 1].wait_recv()
        side = side + side_rcv[d]
    nodes = 2 * own_parents + side.astype(jnp.int32)
    new_nodes[...] = nodes
    node_rcv[0] = nodes

    for j in range(n_rows):
        slots = slice(j * owned, (j + 1) * owned)
        bins_snd[j] = jnp.where(side > 0.5, right_bins[slots, :], left_bins[slots, :])
    for d in range(1, n_rows):
        send(node_rcv.at[0], node_rcv.at[d], node_ss.at[d], node_rs.at[d], at_row(d))
        send(bins_snd.at[partner(d)], bins_rcv.at[d], bins_ss.at[d], bins_rs.at[d], at_row(d))
    bins_rcv[0] = bins_snd[me]

    def wait_for(d):
        for src, dst, ss, rs in (
            (gh, gh_rcv, gh_ss, gh_rs),
            (node_rcv.at[0], node_rcv, node_ss, node_rs),
            (bins_snd.at[0], bins_rcv, bins_ss, bins_rs),
        ):
            pltpu.make_async_remote_copy(
                src_ref=src, dst_ref=dst.at[d], send_sem=ss.at[d], recv_sem=rs.at[d],
                device_id=at_row(1), device_id_type=MESH,
            ).wait()

    bin_sub = lax.broadcasted_iota(jnp.int32, (BINS, rows_here), 0).astype(jnp.float32).astype(jnp.bfloat16)

    def add_source(d):
        there = node_sub == node_rcv[d]
        weights = jnp.concatenate(
            [jnp.where(there, gh_rcv[d, 0:1], 0.0), jnp.where(there, gh_rcv[d, 1:2], 0.0)], axis=0
        ).astype(jnp.bfloat16)
        bins = bins_rcv[d].astype(jnp.bfloat16)
        one = jnp.ones((), jnp.bfloat16)
        none = jnp.zeros((), jnp.bfloat16)
        for k in range(owned):
            le[k * BINS : (k + 1) * BINS, :] = jnp.where(bins[k : k + 1] <= bin_sub, one, none)
        return lax.dot_general(le[...], weights, (((1,), (1,)), ((), ())), preferred_element_type=jnp.float32)

    acc[...] = add_source(0)

    @pl.loop(1, n_rows)
    def _(d):
        wait_for(d)
        acc[...] += add_source(d)

    below = lax.broadcasted_iota(jnp.int32, (BINS, node_count), 0) < BINS - 1
    best = None
    for k in range(owned):
        left_grad = acc[k * BINS : (k + 1) * BINS, 0:node_count]
        left_hess = acc[k * BINS : (k + 1) * BINS, node_count : 2 * node_count]
        total_grad = left_grad[BINS - 1 : BINS]
        total_hess = left_hess[BINS - 1 : BINS]
        right_grad = total_grad - left_grad
        gain = 0.5 * (
            left_grad * left_grad / (left_hess + l2_penalty)
            + right_grad * right_grad / (total_hess - left_hess + l2_penalty)
            - total_grad * total_grad / (total_hess + l2_penalty)
        )
        top = jnp.max(jnp.where(below, gain, -jnp.inf), axis=0, keepdims=True)
        best_out[k : k + 1, :] = top
        best = top if best is None else jnp.maximum(best, top)

    top_snd[...] = best
    sent = []
    for i, (d, e) in enumerate(others):
        sent.append(send(top_snd, top_rcv.at[i], top_ss.at[i], top_rs.at[i], at(d, e)))
    for i, copy in enumerate(sent):
        copy.wait()
        best = jnp.maximum(best, top_rcv[i])
    node_best[...] = best
    for d in range(1, n_rep):
        copies[d - 1].wait_send()


def hand_on(*refs):
    for src, dst in zip(refs[:3], refs[3:]):
        dst[...] = src[...]


def body(n_rows, n_rep, binned, gradients, hessians, parents, split_feature, split_bin, elected):
    rows_here, block_width = binned.shape
    node_count, slots_here = elected.shape
    owned = slots_here // n_rows
    f32 = jnp.float32
    vmem = pl.BlockSpec(memory_space=pltpu.VMEM)
    dma = pltpu.SemaphoreType.DMA
    new_nodes, best, node_best = pl.pallas_call(
        functools.partial(kernel, n_rows, n_rep),
        out_shape=(
            jax.ShapeDtypeStruct((1, rows_here), jnp.int32),
            jax.ShapeDtypeStruct((owned, node_count), f32),
            jax.ShapeDtypeStruct((1, node_count), f32),
        ),
        in_specs=[pl.BlockSpec(memory_space=pl.ANY)] * 7,
        out_specs=(vmem, vmem, vmem),
        scratch_shapes=[
            pltpu.SMEM(split_feature.shape, jnp.int32),
            pltpu.SMEM(split_bin.shape, jnp.int32),
            pltpu.VMEM(binned.shape, jnp.int32),
            pltpu.VMEM(gradients.shape, gradients.dtype),
            pltpu.VMEM(hessians.shape, hessians.dtype),
            pltpu.VMEM((1, rows_here), jnp.int32),
            pltpu.VMEM(elected.shape, jnp.int32),
            dma((7,)),
            pltpu.VMEM((2, rows_here), f32),
            pltpu.VMEM((slots_here, rows_here), f32),
            pltpu.VMEM((slots_here, rows_here), f32),
            pltpu.VMEM((1, rows_here), f32),
            pltpu.VMEM((n_rep, 1, rows_here), f32),
            pltpu.VMEM((n_rows, owned, rows_here), f32),
            pltpu.VMEM((n_rows, owned, rows_here), f32),
            pltpu.VMEM((n_rows, 1, rows_here), jnp.int32),
            pltpu.VMEM((n_rows, 2, rows_here), f32),
            pltpu.VMEM((owned * BINS, rows_here), jnp.bfloat16),
            pltpu.VMEM((owned * BINS, 2 * node_count), f32),
            pltpu.VMEM((1, node_count), f32),
            pltpu.VMEM((n_rows * n_rep - 1, 1, node_count), f32),
        ]
        + [dma((n_rep,))] * 2 + [dma((n_rows,))] * 6 + [dma((n_rows * n_rep - 1,))] * 2,
        compiler_params=pltpu.CompilerParams(collective_id=0, has_side_effects=True),
    )(split_feature, split_bin, binned, gradients, hessians, parents.reshape(1, rows_here), elected)
    made = (new_nodes, best, node_best)
    new_nodes, best, node_best = pl.pallas_call(
        hand_on,
        out_shape=tuple(jax.ShapeDtypeStruct(a.shape, a.dtype) for a in made),
        in_specs=[vmem] * 3,
        out_specs=(vmem,) * 3,
    )(*made)
    return (
        new_nodes.reshape(rows_here),
        best.T.reshape(node_count, 1, owned),
        node_best.reshape(node_count),
    )


def solution(mesh):
    return jax.shard_map(
        functools.partial(body, mesh.shape["rows"], mesh.shape["rep"]),
        mesh=mesh,
        in_specs=(P("rows", "rep"), P("rows"), P("rows"), P("rows"), P(), P(), P(None, "rep")),
        out_specs=(P("rows"), P(None, "rep", "rows"), P()),
        check_vma=False,
    )
```
